32 devices in a mesh: groups: 2 (over x), owner: 16 (over z, y, core).
Axes of the slice: x: 2, y: 2, z: 4, core: 2. Of those that a mesh axis runs over, the one named last changes fastest.
Arguments:
- queries: bfloat16 [2048, 1024], P(('groups', 'owner')), parts along dimension 0, may hold values from -0.3984375 to 0.3984375
- probes: int32 [2048, 8], P(('groups', 'owner')), parts along dimension 0, may hold values from 0 to 255, as said below
- passages: bfloat16 [256, 256, 1024], P('owner'), may hold values from -6 to 6
- centroids: bfloat16 [256, 1024], P('owner'), may hold values from -6 to 6
- counts: int32 [256], P('owner'), may hold values from 1 to 256
Outputs:
- scores: float32 [2048, 8, 256], P(('groups', 'owner')), parts along dimension 0
- visits: int32 [2048], P(('groups', 'owner')), parts along dimension 0
The draws below stay inside these ranges and needn't reach their ends.
There are 2 independent parts, one for each index of `groups`. The reference program is written for one: setup_inputs(seed, part) draws one part's arguments, and reference() takes and returns one part's arrays. A program takes and returns all parts, laid end to end along the dimension named above; an argument that names none is the same for every part. Nothing has to cross between parts.
Inputs may be any that keep to these rules, and one draw needn't show every extreme that they name: Cluster c belongs to owner index c // 16. In each aligned block of 64 queries (the queries of one index of owner) at most 64 probes name clusters of one owner, and in every draw some owners receive exactly 64 probes from every block. A query may name a cluster more than once.
All inputs are finite; a program needn't handle non-finite values.
Results may differ from the reference program's by a relative error of at most 0.0003.
Values may be sent and summed in bfloat16 or wider, within the bound.
A program may use at most 64 MiB of HBM per device.

```python
import jax
import jax.numpy as jnp
from jax import lax

D = 1024
PASSAGES = 256
PROBES = 8
Q_DEV = 64
CL_DEV = 16
QUERIES = 1024
CLUSTERS = 256
CAP = 64


def draw_probes(key, part):
    owner_total = CLUSTERS // CL_DEV
    slot_total = owner_total * CAP
    pick_total = Q_DEV * PROBES
    hot_key, rest_key = jax.random.split(jax.random.fold_in(key, 17))
    shuffled = jax.random.permutation(hot_key, owner_total)
    hotness = (shuffled < owner_total // 8).astype(jnp.int32)
    source_keys = jax.random.split(rest_key, owner_total)

    def one_source(source_key):
        key_prio, key_order, key_local = jax.random.split(source_key, 3)
        positions = jnp.arange(slot_total, dtype=jnp.int32)
        slot_owner = positions // CAP
        priority = jax.random.randint(key_prio, (slot_total,), 0, 1024) + hotness[slot_owner] * 2048
        priority = priority * slot_total + positions
        unused, chosen = lax.top_k(priority, pick_total)
        chosen = jax.random.permutation(key_order, chosen)
        local_ids = jax.random.randint(key_local, (pick_total,), 0, CL_DEV)
        return (chosen // CAP * CL_DEV + local_ids).astype(jnp.int32).reshape(Q_DEV, PROBES)
    return jax.vmap(one_source)(source_keys).reshape(QUERIES, PROBES)


def plant(values, stream_key, least, top_value):
    longest = values.shape.index(max(values.shape))
    spots = []
    for shift in (0, 1):
        where = [jax.random.randint(jax.random.fold_in(stream_key, axis), (), 0, length) for axis, length in enumerate(values.shape)]
        where[longest] = (where[longest] + shift) % values.shape[longest]
        spots.append(tuple(where))
    return values.at[spots[0]].set(least).at[spots[1]].set(top_value)


def steps_of(rng, extent, shards, smallest, high):
    factor_of, own = 1.0, jax.random.fold_in(rng, 6)
    for position, blocks in shards:
        steps = jnp.exp(jax.random.uniform(jax.random.fold_in(own, position), (blocks,), jnp.float32, smallest / len(shards), high / len(shards)))
        factor_of = factor_of * jnp.repeat(steps, extent[position] // blocks).reshape([-1 if axis == position else 1 for axis in range(len(extent))])
    return factor_of


def bell_draw(stream_key, dims, scale, reach, shards=(), kind=jnp.bfloat16):
    drawn = scale * jax.random.normal(stream_key, dims, jnp.float32)
    if shards:
        drawn = drawn * steps_of(stream_key, dims, shards, -0.22, 0.18)
    return jnp.clip(drawn, -reach, reach).astype(kind)


def setup_inputs(seed: int = 0, part: int = 0) -> dict:
    key_of = jax.random.split(jax.random.key(seed), 6)
    part_splits = jax.random.split(jax.random.fold_in(key_of[5], part), 6)
    return {
        "queries": bell_draw(part_splits[0], (QUERIES, D), 0.05, 0.3984375, ((0, 16),)),
        "probes": draw_probes(jax.random.fold_in(jax.random.fold_in(key_of[5], part), 71), part),
        "passages": bell_draw(key_of[2], (CLUSTERS, PASSAGES, D), 1.0, 6.0, ((0, 16),)),
        "centroids": bell_draw(key_of[3], (CLUSTERS, D), 1.0, 6.0, ((0, 16),)),
        "counts": plant(jax.random.randint(key_of[4], (CLUSTERS,), 1, PASSAGES + 1), jax.random.fold_in(key_of[4], 1), 1, PASSAGES).astype(jnp.int32),
    }


def reference(queries, probes, passages, centroids, counts):
    query_count, probe_count = probes.shape
    pair_count = query_count * probe_count
    block_size = 256
    cluster_list = probes.reshape(pair_count // block_size, block_size).astype(jnp.int32)
    query_list = (jnp.arange(pair_count, dtype=jnp.int32) // probe_count).reshape(pair_count // block_size, block_size)

    def score_block(pieces):
        cluster_ids, query_ids = pieces
        query_rows = queries[query_ids].astype(jnp.float32)
        chosen = passages[cluster_ids].astype(jnp.float32)
        direct = jnp.einsum('bd,btd->bt', query_rows, chosen)
        centre = jnp.sum(query_rows * centroids[cluster_ids].astype(jnp.float32), axis=1)
        live_mask = jnp.arange(PASSAGES, dtype=jnp.int32)[None, :] < counts[cluster_ids][:, None]
        return jnp.where(live_mask, direct + centre[:, None], jnp.float32(0.0))

    scores = lax.map(score_block, (cluster_list, query_list)).reshape(query_count, probe_count, PASSAGES)
    visits = jnp.sum(counts[probes], axis=1).astype(jnp.int32)
    return scores, visits
```

```python
import jax
import jax.numpy as jnp
from jax import lax
from jax.experimental import pallas as pl
from jax.experimental.pallas import tpu as pltpu
from jax.sharding import PartitionSpec as P


def routed_body(queries, probes, passages, centroids, counts):
    owner_count = lax.axis_size("owner")
    per_device, probe_count = probes.shape
    local_count, block_span, feature_width = passages.shape
    capacity = 2 * per_device * probe_count // owner_count
    pair_count = per_device * probe_count
    passage_blocks = jnp.transpose(passages, (0, 2, 1))
    flat_probes = probes.reshape(-1)
    target_owner = flat_probes // local_count
    target_local = flat_probes % local_count
    owner_hits = (
        target_owner[:, None] == jnp.arange(owner_count, dtype=jnp.int32)[None, :]
    ).astype(jnp.int32)
    slot_rank = jnp.sum((jnp.cumsum(owner_hits, axis=0) - owner_hits) * owner_hits, axis=1)
    slot_index = target_owner * capacity + slot_rank
    pair_ids = jnp.arange(pair_count, dtype=jnp.int32)
    slot_match = slot_index[None, :] == jnp.arange(owner_count * capacity, dtype=jnp.int32)[:, None]
    slot_filled = jnp.any(slot_match, axis=1)
    source_pair = jnp.sum(jnp.where(slot_match, pair_ids[None, :], 0), axis=1)
    send_rows = jnp.where(
        slot_filled[:, None], queries[source_pair // probe_count], jnp.zeros((), jnp.bfloat16)
    )
    send_ids = jnp.where(slot_filled, target_local[source_pair], -1)
    query_rows = lax.all_to_all(
        send_rows.reshape(owner_count, capacity, feature_width),
        "owner",
        split_axis=0,
        concat_axis=0,
        tiled=True,
    )
    cluster_ids = lax.all_to_all(
        send_ids.reshape(owner_count, capacity), "owner", split_axis=0, concat_axis=0, tiled=True
    )
    source_count, slot_count = cluster_ids.shape
    row_total = source_count * slot_count
    flat_rows = query_rows.reshape(row_total, feature_width)
    flat_ids = cluster_ids.reshape(-1)
    group_ids = jnp.where(flat_ids < 0, 0, flat_ids).astype(jnp.int32)
    cluster_pick = flat_ids[:, None] == jnp.arange(local_count, dtype=jnp.int32)[None, :]
    live_sizes = jnp.sum(jnp.where(cluster_pick, counts[None, :], 0), axis=1)
    group_pick = group_ids[:, None] == jnp.arange(local_count, dtype=jnp.int32)[None, :]
    group_sizes = jnp.sum(group_pick.astype(jnp.int32), axis=0)
    order = jnp.argsort(group_ids, stable=True)
    undo_order = jnp.argsort(order, stable=True)
    sorted_rows = flat_rows[order]
    sorted_scores = lax.ragged_dot(
        sorted_rows, passage_blocks, group_sizes, preferred_element_type=jnp.float32
    )
    own_scores = sorted_scores[undo_order]
    centre_term = jnp.einsum(
        "rd,rd->r", flat_rows, centroids[group_ids], preferred_element_type=jnp.float32
    )
    live_mask = jnp.arange(block_span, dtype=jnp.int32)[None, :] < live_sizes[:, None]
    masked_scores = jnp.where(live_mask, own_scores + centre_term[:, None], 0.0)
    back_scores = lax.all_to_all(
        masked_scores.reshape(source_count, slot_count, block_span),
        "owner",
        split_axis=0,
        concat_axis=0,
        tiled=True,
    )
    back_sizes = lax.all_to_all(
        live_sizes.astype(jnp.float32).reshape(source_count, slot_count),
        "owner",
        split_axis=0,
        concat_axis=0,
        tiled=True,
    )
    flat_scores = back_scores.reshape(owner_count * capacity, block_span)
    scores = flat_scores[slot_index].reshape(per_device, probe_count, block_span)
    pair_sizes = back_sizes.reshape(-1)[slot_index].reshape(per_device, probe_count)
    visits = jnp.sum(pair_sizes, axis=1).astype(jnp.int32)
    return (scores, visits)


LANES = 128
TOP = 32767.0


def owner_kernel(
    n, q_ref, meta_ref, slot_ref, probe_ref, pass_ref, cent_ref, cnt_ref,
    out_ref, vis_ref,
    pass_v, qs, ms, dense, picked, sendb, sends, recvb, recvs, code_s, cnt_s, scale_s,
    pass_sem, qsend, msend, qrecv, mrecv, bsend, ssend, brecv, srecv, loc_sem,
):
    clusters, span, width = pass_ref.shape
    per_device, probe_count, _ = out_ref.shape
    planes = n // 4
    rows = 4 * per_device
    meta_rows, _, lane_count = meta_ref.shape
    cap = lane_count // 4
    half = span // 2
    me = lax.axis_index("owner")
    z = me // 4
    y = (me // 2) % 2
    c = me % 2
    y_dev = z * 4 + (1 - y) * 2 + c
    c_dev = z * 4 + y * 2 + (1 - c)
    has_low = z > 0
    has_high = z < planes - 1

    for k in range(clusters):
        pltpu.make_async_copy(pass_ref.at[k], pass_v.at[k], pass_sem.at[k]).start()

    barrier = pltpu.get_barrier_semaphore()

    def greet(dev):
        pl.semaphore_signal(barrier, inc=1, device_id={"owner": dev})

    greet(y_dev)
    greet(c_dev)

    @pl.when(has_low)
    def _():
        greet(me - 4)

    @pl.when(has_high)
    def _():
        greet(me + 4)

    pl.semaphore_wait(barrier, 2 + jnp.where(has_low, 1, 0) + jnp.where(has_high, 1, 0))

    def pair(s, target, dev, own=False):
        return (
            pltpu.make_async_remote_copy(
                src_ref=meta_ref if own else ms.at[s], dst_ref=ms.at[s],
                send_sem=msend.at[s, target], recv_sem=mrecv.at[s], device_id={"owner": dev},
            ),
            pltpu.make_async_remote_copy(
                src_ref=q_ref if own else qs.at[s], dst_ref=qs.at[s],
                send_sem=qsend.at[s, target], recv_sem=qrecv.at[s], device_id={"owner": dev},
            ),
        )

    def push(s, target, dev, own=False):
        for copy in pair(s, target, dev, own):
            copy.start()

    def drain(s, target, dev, own=False):
        for copy in pair(s, target, dev, own):
            copy.wait_send()

    def arrive(s):
        for copy in pair(s, 0, c_dev):
            copy.wait_recv()

    def onward(act, s, low, high, own=False):
        @pl.when(low)
        def _():
            act(s, 0, me - 4, own)

        @pl.when(high)
        def _():
            act(s, 1, me + 4, own)

        act(s, 2, y_dev, own)
        act(s, 3, c_dev, own)

    onward(push, me, has_low, has_high, True)
    qs[me] = q_ref[...]
    ms[me] = meta_ref[...]

    near = jnp.minimum(z, planes - 1 - z)
    long_side = jnp.where(z < planes - 1 - z, 1, -1)

    def plane_of(k):
        both = jnp.where(k % 2 == 1, -1, 1) * ((k + 1) // 2)
        return z + jnp.where(k <= 2 * near, both, long_side * (k - near))

    def relay_z(k, act=push, wait=True):
        p = plane_of(k)
        s = p * 4 + y * 2 + c
        if wait:
            arrive(s)
        onward(act, s, (p > z) & has_low, (p < z) & has_high)

    def relay_y(k):
        s = plane_of(k) * 4 + (1 - y) * 2 + c
        arrive(s)
        push(s, 3, c_dev)

    def back_pair(s):
        return (
            pltpu.make_async_remote_copy(
                src_ref=sendb.at[s], dst_ref=recvb.at[me],
                send_sem=bsend.at[s], recv_sem=brecv.at[me], device_id={"owner": s},
            ),
            pltpu.make_async_remote_copy(
                src_ref=sends.at[s // 4], dst_ref=recvs.at[me],
                send_sem=ssend.at[s], recv_sem=srecv.at[me], device_id={"owner": s},
            ),
        )

    def to_scalar(s):
        return (
            pltpu.make_async_copy(ms.at[s, me // 4], code_s.at[s], loc_sem.at[0, s]),
            pltpu.make_async_copy(ms.at[s, meta_rows - 1], cnt_s.at[s], loc_sem.at[1, s]),
        )

    def compute(k):
        p = plane_of(k)
        base = p * 4
        for i in range(4):
            for copy in to_scalar(base + i):
                copy.start()
        block = qs[pl.ds(base, 4)].reshape(rows, width)
        centre = lax.dot_general(
            block, cent_ref[...], (((1,), (1,)), ((), ())), preferred_element_type=jnp.float32
        )
        lane = lax.broadcasted_iota(jnp.int32, centre.shape, 1)
        slot_lane = lax.broadcasted_iota(jnp.int32, (1, span), 1)

        def one_cluster(cl, carry):
            @pl.when(k == 0)
            def _():
                pltpu.make_async_copy(pass_ref.at[cl], pass_v.at[cl], pass_sem.at[cl]).wait()

            direct = lax.dot_general(
                qs[pl.ds(base, 4)].reshape(rows, width), pass_v[cl],
                (((1,), (1,)), ((), ())), preferred_element_type=jnp.float32,
            )
            term = jnp.sum(jnp.where(lane == cl, centre, 0.0), axis=1, keepdims=True)
            dense[pl.ds(pl.multiple_of(cl * rows, rows), rows), :] = jnp.where(
                slot_lane < cnt_ref[cl], direct + term, 0.0
            )
            return carry

        lax.fori_loop(0, clusters, one_cluster, 0)
        for i in range(4):
            for copy in to_scalar(base + i):
                copy.wait()
        for i in range(4):
            code_lane = (me % 4) * cap

            def eight(g, carry):
                for u in range(8):
                    k_slot = g * 8 + u
                    row = code_s[base + i, 0, code_lane + k_slot] + i * per_device
                    picked[pl.ds(i * cap + k_slot, 1), :] = dense[pl.ds(row, 1), :]
                return carry

            lax.fori_loop(0, cap // 8, eight, 0)
        found = picked[...]
        top = jnp.maximum(jnp.max(jnp.abs(found), axis=1, keepdims=True), 1e-30)
        coded = jnp.round(found * (TOP / top)).astype(jnp.int32)
        packed = (coded[:, half:] << 16) | (coded[:, :half] & 0xFFFF)
        sendb[pl.ds(base, 4)] = packed.reshape(4, cap, half)
        wide = jnp.broadcast_to(top * (1.0 / TOP), (4 * cap, LANES))
        sends[p] = jnp.transpose(wide)[0:1, :]
        for i in range(4):
            s = base + i

            @pl.when(s == me)
            def _():
                recvb[me] = sendb[me]
                recvs[me] = sends[p]

            @pl.when(s != me)
            def _():
                for copy in back_pair(s):
                    copy.start()

    ahead = 1 + jnp.where(near >= 1, 1, 0)

    def step(k, carry):
        @pl.when((k == 0) & (planes > 1))
        def _():
            relay_z(1)

        @pl.when((k == 0) & (ahead > 1))
        def _():
            relay_z(2)

        @pl.when((k > 0) & (k + ahead < planes))
        def _():
            relay_z(k + ahead)

        relay_y(k)
        p = plane_of(k)
        arrive(p * 4 + y * 2 + (1 - c))
        arrive(p * 4 + (1 - y) * 2 + (1 - c))
        compute(k)
        return carry

    lax.fori_loop(0, planes, step, 0)

    def collect(s, carry):
        @pl.when(s != me)
        def _():
            for copy in (
                pltpu.make_async_remote_copy(
                    src_ref=sendb.at[s], dst_ref=recvb.at[s],
                    send_sem=bsend.at[s], recv_sem=brecv.at[s], device_id={"owner": c_dev},
                ),
                pltpu.make_async_remote_copy(
                    src_ref=sends.at[s // 4], dst_ref=recvs.at[s],
                    send_sem=ssend.at[s], recv_sem=srecv.at[s], device_id={"owner": c_dev},
                ),
            ):
                copy.wait_recv()

        return carry

    lax.fori_loop(0, n, collect, 0)
    scale_copy = pltpu.make_async_copy(recvs, scale_s, loc_sem.at[0, 0])
    scale_copy.start()
    scale_copy.wait()

    def one_query(q, carry):
        visited = jnp.int32(0)
        for j in range(probe_count):
            slot = slot_ref[q * probe_count + j]
            probe = probe_ref[q * probe_count + j]
            owner = slot // cap
            kept = slot % cap
            scale = scale_s[owner, 0, (me % 4) * cap + kept]
            word = recvb[owner, pl.ds(kept, 1), :]
            low = (word << 16) >> 16
            out_ref[q, j : j + 1, :half] = low.astype(jnp.float32) * scale
            out_ref[q, j : j + 1, half:] = (word >> 16).astype(jnp.float32) * scale
            visited = visited + cnt_s[probe // clusters, 0, probe % clusters]
        vis_ref[q] = visited
        return carry

    lax.fori_loop(0, per_device, one_query, 0)

    onward(drain, me, has_low, has_high, True)

    def finish(k, carry):
        @pl.when(k > 0)
        def _():
            relay_z(k, drain, False)

        drain(plane_of(k) * 4 + (1 - y) * 2 + c, 3, c_dev)
        return carry

    lax.fori_loop(0, planes, finish, 0)

    def finish_back(s, carry):
        @pl.when(s != me)
        def _():
            for copy in back_pair(s):
                copy.wait_send()

        return carry

    lax.fori_loop(0, n, finish_back, 0)


def slot_tables(flat_probes, n, cap, clusters, per_device, probe_count):
    pair_count = flat_probes.shape[0]
    owner = flat_probes // clusters
    local = flat_probes % clusters
    pair = jnp.arange(pair_count, dtype=jnp.int32)
    same = (owner[:, None] == owner[None, :]) & (pair[None, :] < pair[:, None])
    slot = owner * cap + jnp.sum(same.astype(jnp.int32), axis=1)
    code = local * (4 * per_device) + pair // probe_count
    hit = slot[None, :] == jnp.arange(n * cap, dtype=jnp.int32)[:, None]
    table = jnp.sum(jnp.where(hit, code[None, :], 0), axis=1)
    return slot, table


def fused_body(queries, probes, passages, centroids, counts):
    n = lax.axis_size("owner")
    per_device, probe_count = probes.shape
    clusters, span, width = passages.shape
    cap = 2 * per_device * probe_count // n
    flat = probes.reshape(-1)
    slot, table = slot_tables(flat, n, cap, clusters, per_device, probe_count)
    lane_count = 4 * cap
    count_row = jnp.pad(counts, (0, lane_count - clusters)).reshape(1, 1, lane_count)
    meta = jnp.concatenate([table.reshape(n // 4, 1, lane_count), count_row], axis=0)
    vmem = pl.BlockSpec(memory_space=pltpu.VMEM)
    smem = pl.BlockSpec(memory_space=pltpu.SMEM)
    dma = pltpu.SemaphoreType.DMA
    rows = 4 * per_device
    half = span // 2
    return pl.pallas_call(
        lambda *refs: owner_kernel(n, *refs),
        out_shape=(
            jax.ShapeDtypeStruct((per_device, probe_count, span), jnp.float32),
            jax.ShapeDtypeStruct((per_device,), jnp.int32),
        ),
        in_specs=[vmem, vmem, smem, smem, pl.BlockSpec(memory_space=pl.ANY), vmem, smem],
        out_specs=(vmem, smem),
        scratch_shapes=[
            pltpu.VMEM((clusters, span, width), jnp.bfloat16),
            pltpu.VMEM((n, per_device, width), jnp.bfloat16),
            pltpu.VMEM((n, n // 4 + 1, 1, lane_count), jnp.int32),
            pltpu.VMEM((clusters * rows, span), jnp.float32),
            pltpu.VMEM((4 * cap, span), jnp.float32),
            pltpu.VMEM((n, cap, half), jnp.int32),
            pltpu.VMEM((n // 4, 1, lane_count), jnp.float32),
            pltpu.VMEM((n, cap, half), jnp.int32),
            pltpu.VMEM((n, 1, lane_count), jnp.float32),
            pltpu.SMEM((n, 1, lane_count), jnp.int32),
            pltpu.SMEM((n, 1, lane_count), jnp.int32),
            pltpu.SMEM((n, 1, lane_count), jnp.float32),
            dma((clusters,)),
            dma((n, 4)),
            dma((n, 4)),
            dma((n,)),
            dma((n,)),
            dma((n,)),
            dma((n,)),
            dma((n,)),
            dma((n,)),
            dma((2, n)),
        ],
        compiler_params=pltpu.CompilerParams(
            collective_id=0, has_side_effects=True, vmem_limit_bytes=48 * 2**20
        ),
    )(queries, meta, slot, flat, passages, centroids, counts)


def body(queries, probes, passages, centroids, counts):
    n = lax.axis_size("owner")
    per_device, probe_count = probes.shape
    clusters, span, width = passages.shape
    lane_count = 8 * per_device * probe_count // n
    held = clusters * span * (2 * width + 16 * per_device) + 2 * n * per_device * width
    fits = (
        n % 4 == 0 and n >= 8 and lane_count % LANES == 0 and lane_count >= clusters
        and span % (2 * LANES) == 0 and held < 32 * 2**20
    )
    chosen = fused_body if fits else routed_body
    return chosen(queries, probes, passages, centroids, counts)


def solution(mesh):
    in_specs = (
        P(("groups", "owner"), None),
        P(("groups", "owner"), None),
        P("owner", None, None),
        P("owner", None),
        P("owner"),
    )
    out_specs = (P(("groups", "owner"), None, None), P(("groups", "owner")))
    return jax.shard_map(body, mesh=mesh, in_specs=in_specs, out_specs=out_specs, check_vma=False)
```

```python
import jax
import jax.numpy as jnp
from jax import lax
from jax.experimental import pallas as pl
from jax.experimental.pallas import tpu as pltpu
from jax.sharding import PartitionSpec as P


def routed_body(queries, probes, passages, centroids, counts):
    owner_count = lax.axis_size("owner")
    per_device, probe_count = probes.shape
    local_count, block_span, feature_width = passages.shape
    capacity = 2 * per_device * probe_count // owner_count
    pair_count = per_device * probe_count
    passage_blocks = jnp.transpose(passages, (0, 2, 1))
    flat_probes = probes.reshape(-1)
    target_owner = flat_probes // local_count
    target_local = flat_probes % local_count
    owner_hits = (
        target_owner[:, None] == jnp.arange(owner_count, dtype=jnp.int32)[None, :]
    ).astype(jnp.int32)
    slot_rank = jnp.sum((jnp.cumsum(owner_hits, axis=0) - owner_hits) * owner_hits, axis=1)
    slot_index = target_owner * capacity + slot_rank
    pair_ids = jnp.arange(pair_count, dtype=jnp.int32)
    slot_match = slot_index[None, :] == jnp.arange(owner_count * capacity, dtype=jnp.int32)[:, None]
    slot_filled = jnp.any(slot_match, axis=1)
    source_pair = jnp.sum(jnp.where(slot_match, pair_ids[None, :], 0), axis=1)
    send_rows = jnp.where(
        slot_filled[:, None], queries[source_pair // probe_count], jnp.zeros((), jnp.bfloat16)
    )
    send_ids = jnp.where(slot_filled, target_local[source_pair], -1)
    query_rows = lax.all_to_all(
        send_rows.reshape(owner_count, capacity, feature_width),
        "owner",
        split_axis=0,
        concat_axis=0,
        tiled=True,
    )
    cluster_ids = lax.all_to_all(
        send_ids.reshape(owner_count, capacity), "owner", split_axis=0, concat_axis=0, tiled=True
    )
    source_count, slot_count = cluster_ids.shape
    row_total = source_count * slot_count
    flat_rows = query_rows.reshape(row_total, feature_width)
    flat_ids = cluster_ids.reshape(-1)
    group_ids = jnp.where(flat_ids < 0, 0, flat_ids).astype(jnp.int32)
    cluster_pick = flat_ids[:, None] == jnp.arange(local_count, dtype=jnp.int32)[None, :]
    live_sizes = jnp.sum(jnp.where(cluster_pick, counts[None, :], 0), axis=1)
    group_pick = group_ids[:, None] == jnp.arange(local_count, dtype=jnp.int32)[None, :]
    group_sizes = jnp.sum(group_pick.astype(jnp.int32), axis=0)
    order = jnp.argsort(group_ids, stable=True)
    undo_order = jnp.argsort(order, stable=True)
    sorted_rows = flat_rows[order]
    sorted_scores = lax.ragged_dot(
        sorted_rows, passage_blocks, group_sizes, preferred_element_type=jnp.float32
    )
    own_scores = sorted_scores[undo_order]
    centre_term = jnp.einsum(
        "rd,rd->r", flat_rows, centroids[group_ids], preferred_element_type=jnp.float32
    )
    live_mask = jnp.arange(block_span, dtype=jnp.int32)[None, :] < live_sizes[:, None]
    masked_scores = jnp.where(live_mask, own_scores + centre_term[:, None], 0.0)
    back_scores = lax.all_to_all(
        masked_scores.reshape(source_count, slot_count, block_span),
        "owner",
        split_axis=0,
        concat_axis=0,
        tiled=True,
    )
    back_sizes = lax.all_to_all(
        live_sizes.astype(jnp.float32).reshape(source_count, slot_count),
        "owner",
        split_axis=0,
        concat_axis=0,
        tiled=True,
    )
    flat_scores = back_scores.reshape(owner_count * capacity, block_span)
    scores = flat_scores[slot_index].reshape(per_device, probe_count, block_span)
    pair_sizes = back_sizes.reshape(-1)[slot_index].reshape(per_device, probe_count)
    visits = jnp.sum(pair_sizes, axis=1).astype(jnp.int32)
    return (scores, visits)


LANES = 128
GROUP = 2
TOP = 32767.0


def owner_kernel(
    n, q_ref, meta_ref, code_ref, pass_ref, cent_ref, cnt_ref,
    out_ref, vis_ref,
    pass_v, qs, ms, dense, picked, sendb, sends, recvb, recvs, words, factors, code_s, cnt_s, scale_s,
    pass_sem, qsend, msend, qrecv, mrecv, bsend, ssend, brecv, srecv, loc_sem,
):
    clusters, span, width = pass_ref.shape
    per_device, probe_count, _ = out_ref.shape
    planes = n // 4
    rows = 4 * per_device
    meta_rows, _, lane_count = meta_ref.shape
    cap = lane_count // 4
    parts = span // LANES
    half = parts // 2
    piece = per_device // 2
    me = lax.axis_index("owner")
    z = me // 4
    y = (me // 2) % 2
    c = me % 2
    y_dev = z * 4 + (1 - y) * 2 + c
    c_dev = z * 4 + y * 2 + (1 - c)
    has_low = z > 0
    has_high = z < planes - 1

    for k in range(clusters):
        pltpu.make_async_copy(pass_ref.at[k], pass_v.at[k], pass_sem.at[k]).start()

    barrier = pltpu.get_barrier_semaphore()

    def greet(dev):
        pl.semaphore_signal(barrier, inc=1, device_id={"owner": dev})

    greet(y_dev)
    greet(c_dev)

    @pl.when(has_low)
    def _():
        greet(me - 4)

    @pl.when(has_high)
    def _():
        greet(me + 4)

    pl.semaphore_wait(barrier, 2 + jnp.where(has_low, 1, 0) + jnp.where(has_high, 1, 0))

    def pair(s, h, target, dev, own=False):
        cut = pl.ds(h * piece, piece)
        query_copy = pltpu.make_async_remote_copy(
            src_ref=q_ref.at[cut] if own else qs.at[s, cut], dst_ref=qs.at[s, cut],
            send_sem=qsend.at[s, h, target], recv_sem=qrecv.at[s, h], device_id={"owner": dev},
        )
        if h == 0:
            return (query_copy,)
        return (
            query_copy,
            pltpu.make_async_remote_copy(
                src_ref=meta_ref if own else ms.at[s], dst_ref=ms.at[s],
                send_sem=msend.at[s, target], recv_sem=mrecv.at[s], device_id={"owner": dev},
            ),
        )

    def push(s, h, target, dev, own=False):
        for copy in pair(s, h, target, dev, own):
            copy.start()

    def drain(s, h, target, dev, own=False):
        for copy in pair(s, h, target, dev, own):
            copy.wait_send()

    def arrive(s, h):
        for copy in pair(s, h, 0, c_dev):
            copy.wait_recv()

    def onward(act, s, h, low, high, own=False):
        @pl.when(low)
        def _():
            act(s, h, 0, me - 4, own)

        @pl.when(high)
        def _():
            act(s, h, 1, me + 4, own)

        act(s, h, 2, y_dev, own)
        act(s, h, 3, c_dev, own)

    for h in range(2):
        onward(push, me, h, has_low, has_high, True)
    qs[me] = q_ref[...]
    ms[me] = meta_ref[...]

    near = jnp.minimum(z, planes - 1 - z)
    long_side = jnp.where(z < planes - 1 - z, 1, -1)

    def plane_of(k):
        both = jnp.where(k % 2 == 1, -1, 1) * ((k + 1) // 2)
        return z + jnp.where(k <= 2 * near, both, long_side * (k - near))

    def relay_z(k, act=push, wait=True):
        p = plane_of(k)
        s = p * 4 + y * 2 + c
        for h in range(2):
            if wait:
                arrive(s, h)
            onward(act, s, h, (p > z) & has_low, (p < z) & has_high)

    def relay_y(k):
        s = plane_of(k) * 4 + (1 - y) * 2 + c
        for h in range(2):
            arrive(s, h)
            push(s, h, 3, c_dev)

    def back_pair(s):
        return (
            pltpu.make_async_remote_copy(
                src_ref=sendb.at[pl.ds(s * cap, cap)], dst_ref=recvb.at[pl.ds(me * cap, cap)],
                send_sem=bsend.at[s], recv_sem=brecv.at[me], device_id={"owner": s},
            ),
            pltpu.make_async_remote_copy(
                src_ref=sends.at[s // 4], dst_ref=recvs.at[me],
                send_sem=ssend.at[s], recv_sem=srecv.at[me], device_id={"owner": s},
            ),
        )

    def to_scalar(s):
        return (
            pltpu.make_async_copy(ms.at[s, me // 4], code_s.at[s], loc_sem.at[0, s]),
            pltpu.make_async_copy(ms.at[s, meta_rows - 1], cnt_s.at[s], loc_sem.at[1, s]),
        )

    def compute(k):
        p = plane_of(k)
        base = p * 4
        for i in range(4):
            for copy in to_scalar(base + i):
                copy.start()
        block = qs[pl.ds(base, 4)].reshape(rows, width)
        centre = lax.dot_general(
            block, cent_ref[...], (((1,), (1,)), ((), ())), preferred_element_type=jnp.float32
        )
        lane = lax.broadcasted_iota(jnp.int32, centre.shape, 1)
        slot_lane = lax.broadcasted_iota(jnp.int32, (1, span), 1)

        def some_clusters(g, carry):
            for u in range(GROUP):
                cl = g * GROUP + u

                @pl.when(k == 0)
                def _():
                    pltpu.make_async_copy(pass_ref.at[cl], pass_v.at[cl], pass_sem.at[cl]).wait()

            for u in range(GROUP):
                cl = g * GROUP + u
                direct = lax.dot_general(
                    qs[pl.ds(base, 4)].reshape(rows, width), pass_v[cl],
                    (((1,), (1,)), ((), ())), preferred_element_type=jnp.float32,
                )
                term = jnp.sum(jnp.where(lane == cl, centre, 0.0), axis=1, keepdims=True)
                scored = jnp.where(slot_lane < cnt_ref[cl], direct + term, 0.0)
                for t in range(parts):
                    dense[pl.ds(cl * rows, rows), t, :] = scored[:, t * LANES : (t + 1) * LANES]
            return carry

        lax.fori_loop(0, clusters // GROUP, some_clusters, 0)
        for i in range(4):
            for copy in to_scalar(base + i):
                copy.wait()
        for i in range(4):
            code_lane = (me % 4) * cap

            def eight(g, carry):
                for u in range(8):
                    k_slot = g * 8 + u
                    row = code_s[base + i, 0, code_lane + k_slot] + i * per_device
                    picked[i * cap + k_slot] = dense[row]
                return carry

            lax.fori_loop(0, cap // 8, eight, 0)
        found = [picked[:, t, :] for t in range(parts)]
        peak = jnp.abs(found[0])
        for t in range(1, parts):
            peak = jnp.maximum(peak, jnp.abs(found[t]))
        top = jnp.maximum(jnp.max(peak, axis=1, keepdims=True), 1e-30)
        gain = TOP / top
        coded = [jnp.round(part * gain).astype(jnp.int32) for part in found]
        for t in range(half):
            sendb[pl.ds(base * cap, 4 * cap), t, :] = (coded[half + t] << 16) | (coded[t] & 0xFFFF)
        wide = jnp.broadcast_to(top * (1.0 / TOP), (4 * cap, LANES))
        sends[p] = jnp.transpose(wide)[0:1, :]
        for i in range(4):
            s = base + i

            @pl.when(s == me)
            def _():
                recvb[pl.ds(me * cap, cap)] = sendb[pl.ds(me * cap, cap)]
                recvs[me] = sends[p]

            @pl.when(s != me)
            def _():
                for copy in back_pair(s):
                    copy.start()

    ahead = 1 + jnp.where(near >= 1, 1, 0)

    def step(k, carry):
        @pl.when((k == 0) & (planes > 1))
        def _():
            relay_z(1)

        @pl.when((k == 0) & (ahead > 1))
        def _():
            relay_z(2)

        @pl.when((k > 0) & (k + ahead < planes))
        def _():
            relay_z(k + ahead)

        relay_y(k)
        p = plane_of(k)
        for h in range(2):
            arrive(p * 4 + y * 2 + (1 - c), h)
            arrive(p * 4 + (1 - y) * 2 + (1 - c), h)
        compute(k)
        return carry

    lax.fori_loop(0, planes, step, 0)

    def collect(s, carry):
        @pl.when(s != me)
        def _():
            for copy in (
                pltpu.make_async_remote_copy(
                    src_ref=sendb.at[pl.ds(s * cap, cap)], dst_ref=recvb.at[pl.ds(s * cap, cap)],
                    send_sem=bsend.at[s], recv_sem=brecv.at[s], device_id={"owner": c_dev},
                ),
                pltpu.make_async_remote_copy(
                    src_ref=sends.at[s // 4], dst_ref=recvs.at[s],
                    send_sem=ssend.at[s], recv_sem=srecv.at[s], device_id={"owner": c_dev},
                ),
            ):
                copy.wait_recv()

        return carry

    def count_query(q, carry):
        visited = jnp.int32(0)
        for j in range(probe_count):
            code = code_ref[q * probe_count + j]
            visited = visited + cnt_s[code >> 16, 0, (code >> 8) & 255]
        vis_ref[q] = visited
        return carry

    lax.fori_loop(0, per_device, count_query, 0)
    lax.fori_loop(0, n, collect, 0)
    scale_copy = pltpu.make_async_copy(recvs, scale_s, loc_sem.at[0, 0])
    scale_copy.start()
    scale_copy.wait()
    scale_lane = (me % 4) * cap

    def pick_query(q, carry):
        for j in range(probe_count):
            code = code_ref[q * probe_count + j]
            kept = code & 255
            words[q * probe_count + j] = recvb[(code >> 16) * cap + kept]
            factors[q * probe_count + j] = jnp.full(
                (1, LANES), scale_s[code >> 16, 0, scale_lane + kept], jnp.float32
            )
        return carry

    lax.fori_loop(0, per_device, pick_query, 0)
    factor = factors[:, 0, :]
    for t in range(half):
        word = words[:, t, :]
        low = ((word << 16) >> 16).astype(jnp.float32) * factor
        high = (word >> 16).astype(jnp.float32) * factor
        shape = (per_device, probe_count, LANES)
        out_ref[:, :, t * LANES : (t + 1) * LANES] = low.reshape(shape)
        out_ref[:, :, (half + t) * LANES : (half + t + 1) * LANES] = high.reshape(shape)

    for h in range(2):
        onward(drain, me, h, has_low, has_high, True)

    def finish(k, carry):
        @pl.when(k > 0)
        def _():
            relay_z(k, drain, False)

        for h in range(2):
            drain(plane_of(k) * 4 + (1 - y) * 2 + c, h, 3, c_dev)
        return carry

    lax.fori_loop(0, planes, finish, 0)

    def finish_back(s, carry):
        @pl.when(s != me)
        def _():
            for copy in back_pair(s):
                copy.wait_send()

        return carry

    lax.fori_loop(0, n, finish_back, 0)


def slot_tables(flat_probes, n, cap, clusters, per_device, probe_count):
    pair_count = flat_probes.shape[0]
    owner = flat_probes // clusters
    local = flat_probes % clusters
    pair = jnp.arange(pair_count, dtype=jnp.int32)
    same = (owner[:, None] == owner[None, :]) & (pair[None, :] < pair[:, None])
    slot = owner * cap + jnp.sum(same.astype(jnp.int32), axis=1)
    code = local * (4 * per_device) + pair // probe_count
    hit = slot[None, :] == jnp.arange(n * cap, dtype=jnp.int32)[:, None]
    table = jnp.sum(jnp.where(hit, code[None, :], 0), axis=1)
    return (owner << 16) | (local << 8) | (slot - owner * cap), table


def fused_body(queries, probes, passages, centroids, counts):
    n = lax.axis_size("owner")
    per_device, probe_count = probes.shape
    clusters, span, width = passages.shape
    cap = 2 * per_device * probe_count // n
    flat = probes.reshape(-1)
    codes, table = slot_tables(flat, n, cap, clusters, per_device, probe_count)
    lane_count = 4 * cap
    count_row = jnp.pad(counts, (0, lane_count - clusters)).reshape(1, 1, lane_count)
    meta = jnp.concatenate([table.reshape(n // 4, 1, lane_count), count_row], axis=0)
    vmem = pl.BlockSpec(memory_space=pltpu.VMEM)
    smem = pl.BlockSpec(memory_space=pltpu.SMEM)
    dma = pltpu.SemaphoreType.DMA
    rows = 4 * per_device
    parts = span // LANES
    return pl.pallas_call(
        lambda *refs: owner_kernel(n, *refs),
        out_shape=(
            jax.ShapeDtypeStruct((per_device, probe_count, span), jnp.float32),
            jax.ShapeDtypeStruct((per_device,), jnp.int32),
        ),
        in_specs=[vmem, vmem, smem, pl.BlockSpec(memory_space=pl.ANY), vmem, smem],
        out_specs=(vmem, smem),
        scratch_shapes=[
            pltpu.VMEM((clusters, span, width), jnp.bfloat16),
            pltpu.VMEM((n, per_device, width), jnp.bfloat16),
            pltpu.VMEM((n, n // 4 + 1, 1, lane_count), jnp.int32),
            pltpu.VMEM((clusters * rows, parts, LANES), jnp.float32),
            pltpu.VMEM((4 * cap, parts, LANES), jnp.float32),
            pltpu.VMEM((n * cap, parts // 2, LANES), jnp.int32),
            pltpu.VMEM((n // 4, 1, lane_count), jnp.float32),
            pltpu.VMEM((n * cap, parts // 2, LANES), jnp.int32),
            pltpu.VMEM((n, 1, lane_count), jnp.float32),
            pltpu.VMEM((per_device * probe_count, parts // 2, LANES), jnp.int32),
            pltpu.VMEM((per_device * probe_count, 1, LANES), jnp.float32),
            pltpu.SMEM((n, 1, lane_count), jnp.int32),
            pltpu.SMEM((n, 1, lane_count), jnp.int32),
            pltpu.SMEM((n, 1, lane_count), jnp.float32),
            dma((clusters,)),
            dma((n, 2, 4)),
            dma((n, 4)),
            dma((n, 2)),
            dma((n,)),
            dma((n,)),
            dma((n,)),
            dma((n,)),
            dma((n,)),
            dma((2, n)),
        ],
        compiler_params=pltpu.CompilerParams(
            collective_id=0, has_side_effects=True, vmem_limit_bytes=48 * 2**20
        ),
    )(queries, meta, codes, passages, centroids, counts)


def body(queries, probes, passages, centroids, counts):
    n = lax.axis_size("owner")
    per_device, probe_count = probes.shape
    clusters, span, width = passages.shape
    lane_count = 8 * per_device * probe_count // n
    held = clusters * span * (2 * width + 16 * per_device) + 2 * n * per_device * width
    fits = (
        n % 4 == 0 and n >= 8 and lane_count % LANES == 0 and lane_count >= clusters
        and span % (2 * LANES) == 0 and clusters % GROUP == 0 and clusters <= 256
        and lane_count <= 1024 and per_device % 32 == 0 and held < 32 * 2**20
    )
    chosen = fused_body if fits else routed_body
    return chosen(queries, probes, passages, centroids, counts)


def solution(mesh):
    in_specs = (
        P(("groups", "owner"), None),
        P(("groups", "owner"), None),
        P("owner", None, None),
        P("owner", None),
        P("owner"),
    )
    out_specs = (P(("groups", "owner"), None, None), P(("groups", "owner")))
    return jax.shard_map(body, mesh=mesh, in_specs=in_specs, out_specs=out_specs, check_vma=False)
```

```python
import jax
import jax.numpy as jnp
from jax import lax
from jax.experimental import pallas as pl
from jax.experimental.pallas import tpu as pltpu
from jax.sharding import PartitionSpec as P


def routed_body(queries, probes, passages, centroids, counts):
    owner_count = lax.axis_size("owner")
    per_device, probe_count = probes.shape
    local_count, block_span, feature_width = passages.shape
    capacity = 2 * per_device * probe_count // owner_count
    pair_count = per_device * probe_count
    passage_blocks = jnp.transpose(passages, (0, 2, 1))
    flat_probes = probes.reshape(-1)
    target_owner = flat_probes // local_count
    target_local = flat_probes % local_count
    owner_hits = (
        target_owner[:, None] == jnp.arange(owner_count, dtype=jnp.int32)[None, :]
    ).astype(jnp.int32)
    slot_rank = jnp.sum((jnp.cumsum(owner_hits, axis=0) - owner_hits) * owner_hits, axis=1)
    slot_index = target_owner * capacity + slot_rank
    pair_ids = jnp.arange(pair_count, dtype=jnp.int32)
    slot_match = slot_index[None, :] == jnp.arange(owner_count * capacity, dtype=jnp.int32)[:, None]
    slot_filled = jnp.any(slot_match, axis=1)
    source_pair = jnp.sum(jnp.where(slot_match, pair_ids[None, :], 0), axis=1)
    send_rows = jnp.where(
        slot_filled[:, None], queries[source_pair // probe_count], jnp.zeros((), jnp.bfloat16)
    )
    send_ids = jnp.where(slot_filled, target_local[source_pair], -1)
    query_rows = lax.all_to_all(
        send_rows.reshape(owner_count, capacity, feature_width),
        "owner",
        split_axis=0,
        concat_axis=0,
        tiled=True,
    )
    cluster_ids = lax.all_to_all(
        send_ids.reshape(owner_count, capacity), "owner", split_axis=0, concat_axis=0, tiled=True
    )
    source_count, slot_count = cluster_ids.shape
    row_total = source_count * slot_count
    flat_rows = query_rows.reshape(row_total, feature_width)
    flat_ids = cluster_ids.reshape(-1)
    group_ids = jnp.where(flat_ids < 0, 0, flat_ids).astype(jnp.int32)
    cluster_pick = flat_ids[:, None] == jnp.arange(local_count, dtype=jnp.int32)[None, :]
    live_sizes = jnp.sum(jnp.where(cluster_pick, counts[None, :], 0), axis=1)
    group_pick = group_ids[:, None] == jnp.arange(local_count, dtype=jnp.int32)[None, :]
    group_sizes = jnp.sum(group_pick.astype(jnp.int32), axis=0)
    order = jnp.argsort(group_ids, stable=True)
    undo_order = jnp.argsort(order, stable=True)
    sorted_rows = flat_rows[order]
    sorted_scores = lax.ragged_dot(
        sorted_rows, passage_blocks, group_sizes, preferred_element_type=jnp.float32
    )
    own_scores = sorted_scores[undo_order]
    centre_term = jnp.einsum(
        "rd,rd->r", flat_rows, centroids[group_ids], preferred_element_type=jnp.float32
    )
    live_mask = jnp.arange(block_span, dtype=jnp.int32)[None, :] < live_sizes[:, None]
    masked_scores = jnp.where(live_mask, own_scores + centre_term[:, None], 0.0)
    back_scores = lax.all_to_all(
        masked_scores.reshape(source_count, slot_count, block_span),
        "owner",
        split_axis=0,
        concat_axis=0,
        tiled=True,
    )
    back_sizes = lax.all_to_all(
        live_sizes.astype(jnp.float32).reshape(source_count, slot_count),
        "owner",
        split_axis=0,
        concat_axis=0,
        tiled=True,
    )
    flat_scores = back_scores.reshape(owner_count * capacity, block_span)
    scores = flat_scores[slot_index].reshape(per_device, probe_count, block_span)
    pair_sizes = back_sizes.reshape(-1)[slot_index].reshape(per_device, probe_count)
    visits = jnp.sum(pair_sizes, axis=1).astype(jnp.int32)
    return (scores, visits)


LANES = 128
GROUP = 2
TOP = 32767.0


def owner_kernel(
    n, q_ref, meta_ref, code_ref, pass_ref, cent_ref, cnt_ref,
    out_ref, vis_ref,
    pass_v, qs, ms, dense, picked, sendb, sends, recvb, recvs, words, factors, code_s, cnt_s, scale_s,
    pass_sem, qsend, msend, qrecv, mrecv, bsend, ssend, brecv, srecv, loc_sem,
):
    clusters, span, width = pass_ref.shape
    per_device, probe_count, _ = out_ref.shape
    planes = n // 4
    rows = 4 * per_device
    meta_rows, _, lane_count = meta_ref.shape
    cap = lane_count // 4
    parts = span // LANES
    half = parts // 2
    piece = per_device // 2
    me = lax.axis_index("owner")
    z = me // 4
    y = (me // 2) % 2
    c = me % 2
    y_dev = z * 4 + (1 - y) * 2 + c
    c_dev = z * 4 + y * 2 + (1 - c)

    for k in range(clusters):
        pltpu.make_async_copy(pass_ref.at[k], pass_v.at[k], pass_sem.at[k]).start()

    barrier = pltpu.get_barrier_semaphore()

    def greet(dev):
        pl.semaphore_signal(barrier, inc=1, device_id={"owner": dev})

    greet(y_dev)
    greet(c_dev)

    for p in range(planes):
        @pl.when(p != z)
        def _():
            greet(p * 4 + y * 2 + c)

    pl.semaphore_wait(barrier, planes + 1)

    def pair(s, h, target, dev, own=False):
        cut = pl.ds(h * piece, piece)
        query_copy = pltpu.make_async_remote_copy(
            src_ref=q_ref.at[cut] if own else qs.at[s, cut], dst_ref=qs.at[s, cut],
            send_sem=qsend.at[s, h, target], recv_sem=qrecv.at[s, h], device_id={"owner": dev},
        )
        if h == 0:
            return (query_copy,)
        return (
            query_copy,
            pltpu.make_async_remote_copy(
                src_ref=meta_ref if own else ms.at[s], dst_ref=ms.at[s],
                send_sem=msend.at[s, target], recv_sem=mrecv.at[s], device_id={"owner": dev},
            ),
        )

    def push(s, h, target, dev, own=False):
        for copy in pair(s, h, target, dev, own):
            copy.start()

    def drain(s, h, target, dev, own=False):
        for copy in pair(s, h, target, dev, own):
            copy.wait_send()

    def arrive(s, h):
        for copy in pair(s, h, 0, c_dev):
            copy.wait_recv()

    def onward(act, s, h, own=False):
        act(s, h, planes, y_dev, own)
        act(s, h, planes + 1, c_dev, own)

    def spread(act):
        for h in range(2):
            onward(act, me, h, True)
        for d in range(1, planes):
            for p in (z - d, z + d):
                @pl.when((p >= 0) & (p < planes))
                def _():
                    for h in range(2):
                        act(me, h, p, p * 4 + y * 2 + c, True)

    spread(push)
    qs[me] = q_ref[...]
    ms[me] = meta_ref[...]

    near = jnp.minimum(z, planes - 1 - z)
    long_side = jnp.where(z < planes - 1 - z, 1, -1)

    def plane_of(k):
        both = jnp.where(k % 2 == 1, -1, 1) * ((k + 1) // 2)
        return z + jnp.where(k <= 2 * near, both, long_side * (k - near))

    def relay_z(k, act=push, wait=True):
        p = plane_of(k)
        s = p * 4 + y * 2 + c
        for h in range(2):
            if wait:
                arrive(s, h)
            onward(act, s, h)

    def relay_y(k):
        s = plane_of(k) * 4 + (1 - y) * 2 + c
        for h in range(2):
            arrive(s, h)
            push(s, h, planes + 1, c_dev)

    def back_pair(s):
        return (
            pltpu.make_async_remote_copy(
                src_ref=sendb.at[pl.ds(s * cap, cap)], dst_ref=recvb.at[pl.ds(me * cap, cap)],
                send_sem=bsend.at[s], recv_sem=brecv.at[me], device_id={"owner": s},
            ),
            pltpu.make_async_remote_copy(
                src_ref=sends.at[s // 4], dst_ref=recvs.at[me],
                send_sem=ssend.at[s], recv_sem=srecv.at[me], device_id={"owner": s},
            ),
        )

    def to_scalar(p):
        return pltpu.make_async_copy(
            ms.at[pl.ds(p * 4, 4), me // 4], code_s.at[pl.ds(p * 4, 4)], loc_sem.at[p]
        )

    def compute(k):
        p = plane_of(k)
        base = p * 4
        to_scalar(p).start()
        block = qs[pl.ds(base, 4)].reshape(rows, width)
        centre = lax.dot_general(
            block, cent_ref[...], (((1,), (1,)), ((), ())), preferred_element_type=jnp.float32
        )
        lane = lax.broadcasted_iota(jnp.int32, centre.shape, 1)
        slot_lane = lax.broadcasted_iota(jnp.int32, (1, span), 1)

        def some_clusters(g, carry):
            for u in range(GROUP):
                cl = g * GROUP + u

                @pl.when(k == 0)
                def _():
                    pltpu.make_async_copy(pass_ref.at[cl], pass_v.at[cl], pass_sem.at[cl]).wait()

            for u in range(GROUP):
                cl = g * GROUP + u
                direct = lax.dot_general(
                    qs[pl.ds(base, 4)].reshape(rows, width), pass_v[cl],
                    (((1,), (1,)), ((), ())), preferred_element_type=jnp.float32,
                )
                term = jnp.sum(jnp.where(lane == cl, centre, 0.0), axis=1, keepdims=True)
                scored = jnp.where(slot_lane < cnt_ref[cl], direct + term, 0.0)
                for t in range(parts):
                    dense[pl.ds(cl * rows, rows), t, :] = scored[:, t * LANES : (t + 1) * LANES]
            return carry

        lax.fori_loop(0, clusters // GROUP, some_clusters, 0)
        to_scalar(p).wait()
        for i in range(4):
            code_lane = (me % 4) * cap

            def eight(g, carry):
                for u in range(8):
                    k_slot = g * 8 + u
                    row = code_s[base + i, 0, code_lane + k_slot] + i * per_device
                    picked[i * cap + k_slot] = dense[row]
                return carry

            lax.fori_loop(0, cap // 8, eight, 0)
        found = [picked[:, t, :] for t in range(parts)]
        peak = jnp.abs(found[0])
        for t in range(1, parts):
            peak = jnp.maximum(peak, jnp.abs(found[t]))
        top = jnp.maximum(jnp.max(peak, axis=1, keepdims=True), 1e-30)
        gain = TOP / top
        coded = [jnp.round(part * gain).astype(jnp.int32) for part in found]
        for t in range(half):
            sendb[pl.ds(base * cap, 4 * cap), t, :] = (coded[half + t] << 16) | (coded[t] & 0xFFFF)
        wide = jnp.broadcast_to(top * (1.0 / TOP), (4 * cap, LANES))
        sends[p] = jnp.transpose(wide)[0:1, :]
        for i in range(4):
            s = base + i

            @pl.when(s == me)
            def _():
                recvb[pl.ds(me * cap, cap)] = sendb[pl.ds(me * cap, cap)]
                recvs[me] = sends[p]

            @pl.when(s != me)
            def _():
                for copy in back_pair(s):
                    copy.start()

    def step(k, carry):
        @pl.when(k + 1 < planes)
        def _():
            relay_z(k + 1)

        relay_y(k)
        p = plane_of(k)
        for h in range(2):
            arrive(p * 4 + y * 2 + (1 - c), h)
            arrive(p * 4 + (1 - y) * 2 + (1 - c), h)
        compute(k)
        return carry

    lax.fori_loop(0, planes, step, 0)

    def collect(s, carry):
        @pl.when(s != me)
        def _():
            for copy in (
                pltpu.make_async_remote_copy(
                    src_ref=sendb.at[pl.ds(s * cap, cap)], dst_ref=recvb.at[pl.ds(s * cap, cap)],
                    send_sem=bsend.at[s], recv_sem=brecv.at[s], device_id={"owner": c_dev},
                ),
                pltpu.make_async_remote_copy(
                    src_ref=sends.at[s // 4], dst_ref=recvs.at[s],
                    send_sem=ssend.at[s], recv_sem=srecv.at[s], device_id={"owner": c_dev},
                ),
            ):
                copy.wait_recv()

        return carry

    def count_query(q, carry):
        visited = jnp.int32(0)
        for j in range(probe_count):
            code = code_ref[q * probe_count + j]
            visited = visited + cnt_s[code >> 16, 0, (code >> 8) & 255]
        vis_ref[q] = visited
        return carry

    count_copy = pltpu.make_async_copy(ms.at[:, meta_rows - 1], cnt_s, loc_sem.at[0])
    count_copy.start()
    count_copy.wait()
    lax.fori_loop(0, per_device, count_query, 0)
    lax.fori_loop(0, n, collect, 0)
    scale_copy = pltpu.make_async_copy(recvs, scale_s, loc_sem.at[0])
    scale_copy.start()
    scale_copy.wait()
    scale_lane = (me % 4) * cap

    def pick_query(q, carry):
        for j in range(probe_count):
            code = code_ref[q * probe_count + j]
            kept = code & 255
            words[q * probe_count + j] = recvb[(code >> 16) * cap + kept]
            factors[q * probe_count + j] = jnp.full(
                (1, LANES), scale_s[code >> 16, 0, scale_lane + kept], jnp.float32
            )
        return carry

    lax.fori_loop(0, per_device, pick_query, 0)
    factor = factors[:, 0, :]
    for t in range(half):
        word = words[:, t, :]
        low = ((word << 16) >> 16).astype(jnp.float32) * factor
        high = (word >> 16).astype(jnp.float32) * factor
        shape = (per_device, probe_count, LANES)
        out_ref[:, :, t * LANES : (t + 1) * LANES] = low.reshape(shape)
        out_ref[:, :, (half + t) * LANES : (half + t + 1) * LANES] = high.reshape(shape)

    spread(drain)

    def finish(k, carry):
        @pl.when(k > 0)
        def _():
            relay_z(k, drain, False)

        for h in range(2):
            drain(plane_of(k) * 4 + (1 - y) * 2 + c, h, planes + 1, c_dev)
        return carry

    lax.fori_loop(0, planes, finish, 0)

    def finish_back(s, carry):
        @pl.when(s != me)
        def _():
            for copy in back_pair(s):
                copy.wait_send()

        return carry

    lax.fori_loop(0, n, finish_back, 0)


def slot_tables(flat_probes, n, cap, clusters, per_device, probe_count):
    pair_count = flat_probes.shape[0]
    owner = flat_probes // clusters
    local = flat_probes % clusters
    pair = jnp.arange(pair_count, dtype=jnp.int32)
    same = (owner[:, None] == owner[None, :]) & (pair[None, :] < pair[:, None])
    slot = owner * cap + jnp.sum(same.astype(jnp.int32), axis=1)
    code = local * (4 * per_device) + pair // probe_count
    hit = slot[None, :] == jnp.arange(n * cap, dtype=jnp.int32)[:, None]
    table = jnp.sum(jnp.where(hit, code[None, :], 0), axis=1)
    return (owner << 16) | (local << 8) | (slot - owner * cap), table


def fused_body(queries, probes, passages, centroids, counts):
    n = lax.axis_size("owner")
    per_device, probe_count = probes.shape
    clusters, span, width = passages.shape
    cap = 2 * per_device * probe_count // n
    flat = probes.reshape(-1)
    codes, table = slot_tables(flat, n, cap, clusters, per_device, probe_count)
    lane_count = 4 * cap
    count_row = jnp.pad(counts, (0, lane_count - clusters)).reshape(1, 1, lane_count)
    meta = jnp.concatenate([table.reshape(n // 4, 1, lane_count), count_row], axis=0)
    vmem = pl.BlockSpec(memory_space=pltpu.VMEM)
    smem = pl.BlockSpec(memory_space=pltpu.SMEM)
    dma = pltpu.SemaphoreType.DMA
    rows = 4 * per_device
    parts = span // LANES
    return pl.pallas_call(
        lambda *refs: owner_kernel(n, *refs),
        out_shape=(
            jax.ShapeDtypeStruct((per_device, probe_count, span), jnp.float32),
            jax.ShapeDtypeStruct((per_device,), jnp.int32),
        ),
        in_specs=[vmem, vmem, smem, pl.BlockSpec(memory_space=pl.ANY), vmem, smem],
        out_specs=(vmem, smem),
        scratch_shapes=[
            pltpu.VMEM((clusters, span, width), jnp.bfloat16),
            pltpu.VMEM((n, per_device, width), jnp.bfloat16),
            pltpu.VMEM((n, n // 4 + 1, 1, lane_count), jnp.int32),
            pltpu.VMEM((clusters * rows, parts, LANES), jnp.float32),
            pltpu.VMEM((4 * cap, parts, LANES), jnp.float32),
            pltpu.VMEM((n * cap, parts // 2, LANES), jnp.int32),
            pltpu.VMEM((n // 4, 1, lane_count), jnp.float32),
            pltpu.VMEM((n * cap, parts // 2, LANES), jnp.int32),
            pltpu.VMEM((n, 1, lane_count), jnp.float32),
            pltpu.VMEM((per_device * probe_count, parts // 2, LANES), jnp.int32),
            pltpu.VMEM((per_device * probe_count, 1, LANES), jnp.float32),
            pltpu.SMEM((n, 1, lane_count), jnp.int32),
            pltpu.SMEM((n, 1, lane_count), jnp.int32),
            pltpu.SMEM((n, 1, lane_count), jnp.float32),
            dma((clusters,)),
            dma((n, 2, n // 4 + 2)),
            dma((n, n // 4 + 2)),
            dma((n, 2)),
            dma((n,)),
            dma((n,)),
            dma((n,)),
            dma((n,)),
            dma((n,)),
            dma((n // 4,)),
        ],
        compiler_params=pltpu.CompilerParams(
            collective_id=0, has_side_effects=True, vmem_limit_bytes=48 * 2**20
        ),
    )(queries, meta, codes, passages, centroids, counts)


def body(queries, probes, passages, centroids, counts):
    n = lax.axis_size("owner")
    per_device, probe_count = probes.shape
    clusters, span, width = passages.shape
    lane_count = 8 * per_device * probe_count // n
    held = clusters * span * (2 * width + 16 * per_device) + 2 * n * per_device * width
    fits = (
        n % 4 == 0 and n >= 8 and lane_count % LANES == 0 and lane_count >= clusters
        and span % (2 * LANES) == 0 and clusters % GROUP == 0 and clusters <= 256
        and lane_count <= 1024 and per_device % 32 == 0 and held < 32 * 2**20
    )
    chosen = fused_body if fits else routed_body
    return chosen(queries, probes, passages, centroids, counts)


def solution(mesh):
    in_specs = (
        P(("groups", "owner"), None),
        P(("groups", "owner"), None),
        P("owner", None, None),
        P("owner", None),
        P("owner"),
    )
    out_specs = (P(("groups", "owner"), None, None), P(("groups", "owner")))
    return jax.shard_map(body, mesh=mesh, in_specs=in_specs, out_specs=out_specs, check_vma=False)
```

```python
import jax
import jax.numpy as jnp
from jax import lax
from jax.experimental import pallas as pl
from jax.experimental.pallas import tpu as pltpu
from jax.sharding import PartitionSpec as P


def routed_body(queries, probes, passages, centroids, counts):
    owner_count = lax.axis_size("owner")
    per_device, probe_count = probes.shape
    local_count, block_span, feature_width = passages.shape
    capacity = 2 * per_device * probe_count // owner_count
    pair_count = per_device * probe_count
    passage_blocks = jnp.transpose(passages, (0, 2, 1))
    flat_probes = probes.reshape(-1)
    target_owner = flat_probes // local_count
    target_local = flat_probes % local_count
    owner_hits = (
        target_owner[:, None] == jnp.arange(owner_count, dtype=jnp.int32)[None, :]
    ).astype(jnp.int32)
    slot_rank = jnp.sum((jnp.cumsum(owner_hits, axis=0) - owner_hits) * owner_hits, axis=1)
    slot_index = target_owner * capacity + slot_rank
    pair_ids = jnp.arange(pair_count, dtype=jnp.int32)
    slot_match = slot_index[None, :] == jnp.arange(owner_count * capacity, dtype=jnp.int32)[:, None]
    slot_filled = jnp.any(slot_match, axis=1)
    source_pair = jnp.sum(jnp.where(slot_match, pair_ids[None, :], 0), axis=1)
    send_rows = jnp.where(
        slot_filled[:, None], queries[source_pair // probe_count], jnp.zeros((), jnp.bfloat16)
    )
    send_ids = jnp.where(slot_filled, target_local[source_pair], -1)
    query_rows = lax.all_to_all(
        send_rows.reshape(owner_count, capacity, feature_width),
        "owner",
        split_axis=0,
        concat_axis=0,
        tiled=True,
    )
    cluster_ids = lax.all_to_all(
        send_ids.reshape(owner_count, capacity), "owner", split_axis=0, concat_axis=0, tiled=True
    )
    source_count, slot_count = cluster_ids.shape
    row_total = source_count * slot_count
    flat_rows = query_rows.reshape(row_total, feature_width)
    flat_ids = cluster_ids.reshape(-1)
    group_ids = jnp.where(flat_ids < 0, 0, flat_ids).astype(jnp.int32)
    cluster_pick = flat_ids[:, None] == jnp.arange(local_count, dtype=jnp.int32)[None, :]
    live_sizes = jnp.sum(jnp.where(cluster_pick, counts[None, :], 0), axis=1)
    group_pick = group_ids[:, None] == jnp.arange(local_count, dtype=jnp.int32)[None, :]
    group_sizes = jnp.sum(group_pick.astype(jnp.int32), axis=0)
    order = jnp.argsort(group_ids, stable=True)
    undo_order = jnp.argsort(order, stable=True)
    sorted_rows = flat_rows[order]
    sorted_scores = lax.ragged_dot(
        sorted_rows, passage_blocks, group_sizes, preferred_element_type=jnp.float32
    )
    own_scores = sorted_scores[undo_order]
    centre_term = jnp.einsum(
        "rd,rd->r", flat_rows, centroids[group_ids], preferred_element_type=jnp.float32
    )
    live_mask = jnp.arange(block_span, dtype=jnp.int32)[None, :] < live_sizes[:, None]
    masked_scores = jnp.where(live_mask, own_scores + centre_term[:, None], 0.0)
    back_scores = lax.all_to_all(
        masked_scores.reshape(source_count, slot_count, block_span),
        "owner",
        split_axis=0,
        concat_axis=0,
        tiled=True,
    )
    back_sizes = lax.all_to_all(
        live_sizes.astype(jnp.float32).reshape(source_count, slot_count),
        "owner",
        split_axis=0,
        concat_axis=0,
        tiled=True,
    )
    flat_scores = back_scores.reshape(owner_count * capacity, block_span)
    scores = flat_scores[slot_index].reshape(per_device, probe_count, block_span)
    pair_sizes = back_sizes.reshape(-1)[slot_index].reshape(per_device, probe_count)
    visits = jnp.sum(pair_sizes, axis=1).astype(jnp.int32)
    return (scores, visits)


LANES = 128
TOP = 32767.0


def owner_kernel(
    n, q_ref, meta_ref, code_ref, pass_ref, cent_ref, cnt_ref,
    out_ref, vis_ref,
    pass_v, qs, ms, dense, picked, sendb, sends, recvb, recvs, words, factors, code_s, cnt_s, scale_s,
    pass_sem, qsend, msend, qrecv, mrecv, bsend, ssend, brecv, srecv, loc_sem,
):
    clusters, span, width = pass_ref.shape
    per_device, probe_count, _ = out_ref.shape
    planes = n // 4
    rows = n * per_device
    meta_rows, _, lane_count = meta_ref.shape
    cap = lane_count // 4
    parts = span // LANES
    half = parts // 2
    piece = per_device // 2
    me = lax.axis_index("owner")
    z = me // 4
    y = (me // 2) % 2
    c = me % 2
    y_dev = z * 4 + (1 - y) * 2 + c
    c_dev = z * 4 + y * 2 + (1 - c)
    has_low = z > 0
    has_high = z < planes - 1

    for k in range(clusters):
        pltpu.make_async_copy(pass_ref.at[k], pass_v.at[k], pass_sem.at[k]).start()

    barrier = pltpu.get_barrier_semaphore()

    def greet(dev):
        pl.semaphore_signal(barrier, inc=1, device_id={"owner": dev})

    greet(y_dev)
    greet(c_dev)

    @pl.when(has_low)
    def _():
        greet(me - 4)

    @pl.when(has_high)
    def _():
        greet(me + 4)

    pl.semaphore_wait(barrier, 2 + jnp.where(has_low, 1, 0) + jnp.where(has_high, 1, 0))

    def pair(s, h, target, dev, own=False):
        cut = pl.ds(h * piece, piece)
        query_copy = pltpu.make_async_remote_copy(
            src_ref=q_ref.at[cut] if own else qs.at[s, cut], dst_ref=qs.at[s, cut],
            send_sem=qsend.at[s, h, target], recv_sem=qrecv.at[s, h], device_id={"owner": dev},
        )
        if h == 0:
            return (query_copy,)
        return (
            query_copy,
            pltpu.make_async_remote_copy(
                src_ref=meta_ref if own else ms.at[s], dst_ref=ms.at[s],
                send_sem=msend.at[s, target], recv_sem=mrecv.at[s], device_id={"owner": dev},
            ),
        )

    def push(s, h, target, dev, own=False):
        for copy in pair(s, h, target, dev, own):
            copy.start()

    def drain(s, h, target, dev, own=False):
        for copy in pair(s, h, target, dev, own):
            copy.wait_send()

    def arrive(s, h):
        for copy in pair(s, h, 0, c_dev):
            copy.wait_recv()

    def onward(act, s, h, low, high, own=False):
        @pl.when(low)
        def _():
            act(s, h, 0, me - 4, own)

        @pl.when(high)
        def _():
            act(s, h, 1, me + 4, own)

        act(s, h, 2, y_dev, own)
        act(s, h, 3, c_dev, own)

    for h in range(2):
        onward(push, me, h, has_low, has_high, True)
    qs[me] = q_ref[...]
    ms[me] = meta_ref[...]

    near = jnp.minimum(z, planes - 1 - z)
    long_side = jnp.where(z < planes - 1 - z, 1, -1)

    def plane_of(k):
        both = jnp.where(k % 2 == 1, -1, 1) * ((k + 1) // 2)
        return z + jnp.where(k <= 2 * near, both, long_side * (k - near))

    def relay_z(k, act=push, wait=True):
        p = plane_of(k)
        s = p * 4 + y * 2 + c
        for h in range(2):
            if wait:
                arrive(s, h)
            onward(act, s, h, (p > z) & has_low, (p < z) & has_high)

    def relay_y(k):
        s = plane_of(k) * 4 + (1 - y) * 2 + c
        for h in range(2):
            arrive(s, h)
            push(s, h, 3, c_dev)

    def back_pair(s):
        return (
            pltpu.make_async_remote_copy(
                src_ref=sendb.at[pl.ds(s * cap, cap)], dst_ref=recvb.at[pl.ds(me * cap, cap)],
                send_sem=bsend.at[s], recv_sem=brecv.at[me], device_id={"owner": s},
            ),
            pltpu.make_async_remote_copy(
                src_ref=sends.at[s // 4], dst_ref=recvs.at[me],
                send_sem=ssend.at[s], recv_sem=srecv.at[me], device_id={"owner": s},
            ),
        )

    def to_scalar(p):
        return pltpu.make_async_copy(
            ms.at[pl.ds(p * 4, 4), me // 4], code_s.at[pl.ds(p * 4, 4)], loc_sem.at[p]
        )

    def multiply():
        block = qs[...].reshape(rows, width)
        centre = lax.dot_general(
            block, cent_ref[...], (((1,), (1,)), ((), ())), preferred_element_type=jnp.float32
        )
        lane = lax.broadcasted_iota(jnp.int32, centre.shape, 1)
        slot_lane = lax.broadcasted_iota(jnp.int32, (1, span), 1)

        def one_cluster(cl, carry):
            pltpu.make_async_copy(pass_ref.at[cl], pass_v.at[cl], pass_sem.at[cl]).wait()
            direct = lax.dot_general(
                qs[...].reshape(rows, width), pass_v[cl],
                (((1,), (1,)), ((), ())), preferred_element_type=jnp.float32,
            )
            term = jnp.sum(jnp.where(lane == cl, centre, 0.0), axis=1, keepdims=True)
            scored = jnp.where(slot_lane < cnt_ref[cl], direct + term, 0.0)
            for t in range(parts):
                dense[pl.ds(cl * rows, rows), t, :] = scored[:, t * LANES : (t + 1) * LANES]
            return carry

        lax.fori_loop(0, clusters, one_cluster, 0)

    def compute(k):
        p = plane_of(planes - 1 - k)
        base = p * 4
        to_scalar(p).wait()
        for i in range(4):
            code_lane = (me % 4) * cap

            def eight(g, carry):
                for u in range(8):
                    k_slot = g * 8 + u
                    row = code_s[base + i, 0, code_lane + k_slot] + (base + i) * per_device
                    picked[i * cap + k_slot] = dense[row]
                return carry

            lax.fori_loop(0, cap // 8, eight, 0)
        found = [picked[:, t, :] for t in range(parts)]
        peak = jnp.abs(found[0])
        for t in range(1, parts):
            peak = jnp.maximum(peak, jnp.abs(found[t]))
        top = jnp.maximum(jnp.max(peak, axis=1, keepdims=True), 1e-30)
        gain = TOP / top
        coded = [jnp.round(part * gain).astype(jnp.int32) for part in found]
        for t in range(half):
            sendb[pl.ds(base * cap, 4 * cap), t, :] = (coded[half + t] << 16) | (coded[t] & 0xFFFF)
        wide = jnp.broadcast_to(top * (1.0 / TOP), (4 * cap, LANES))
        sends[p] = jnp.transpose(wide)[0:1, :]
        for i in range(4):
            s = base + i

            @pl.when(s == me)
            def _():
                recvb[pl.ds(me * cap, cap)] = sendb[pl.ds(me * cap, cap)]
                recvs[me] = sends[p]

            @pl.when(s != me)
            def _():
                for copy in back_pair(s):
                    copy.start()

    ahead = 1 + jnp.where(near >= 1, 1, 0)

    def step(k, carry):
        @pl.when((k == 0) & (planes > 1))
        def _():
            relay_z(1)

        @pl.when((k == 0) & (ahead > 1))
        def _():
            relay_z(2)

        @pl.when((k > 0) & (k + ahead < planes))
        def _():
            relay_z(k + ahead)

        relay_y(k)
        p = plane_of(k)
        for h in range(2):
            arrive(p * 4 + y * 2 + (1 - c), h)
            arrive(p * 4 + (1 - y) * 2 + (1 - c), h)
        to_scalar(p).start()
        return carry

    lax.fori_loop(0, planes, step, 0)
    multiply()

    def answer(k, carry):
        compute(k)
        return carry

    lax.fori_loop(0, planes, answer, 0)

    def collect(s, carry):
        @pl.when(s != me)
        def _():
            for copy in (
                pltpu.make_async_remote_copy(
                    src_ref=sendb.at[pl.ds(s * cap, cap)], dst_ref=recvb.at[pl.ds(s * cap, cap)],
                    send_sem=bsend.at[s], recv_sem=brecv.at[s], device_id={"owner": c_dev},
                ),
                pltpu.make_async_remote_copy(
                    src_ref=sends.at[s // 4], dst_ref=recvs.at[s],
                    send_sem=ssend.at[s], recv_sem=srecv.at[s], device_id={"owner": c_dev},
                ),
            ):
                copy.wait_recv()

        return carry

    def count_query(q, carry):
        visited = jnp.int32(0)
        for j in range(probe_count):
            code = code_ref[q * probe_count + j]
            visited = visited + cnt_s[code >> 16, 0, (code >> 8) & 255]
        vis_ref[q] = visited
        return carry

    count_copy = pltpu.make_async_copy(ms.at[:, meta_rows - 1], cnt_s, loc_sem.at[0])
    count_copy.start()
    count_copy.wait()
    lax.fori_loop(0, per_device, count_query, 0)
    lax.fori_loop(0, n, collect, 0)
    scale_copy = pltpu.make_async_copy(recvs, scale_s, loc_sem.at[0])
    scale_copy.start()
    scale_copy.wait()
    scale_lane = (me % 4) * cap

    def pick_query(q, carry):
        for j in range(probe_count):
            code = code_ref[q * probe_count + j]
            kept = code & 255
            words[q * probe_count + j] = recvb[(code >> 16) * cap + kept]
            factors[q * probe_count + j] = jnp.full(
                (1, LANES), scale_s[code >> 16, 0, scale_lane + kept], jnp.float32
            )
        return carry

    lax.fori_loop(0, per_device, pick_query, 0)
    factor = factors[:, 0, :]
    for t in range(half):
        word = words[:, t, :]
        low = ((word << 16) >> 16).astype(jnp.float32) * factor
        high = (word >> 16).astype(jnp.float32) * factor
        shape = (per_device, probe_count, LANES)
        out_ref[:, :, t * LANES : (t + 1) * LANES] = low.reshape(shape)
        out_ref[:, :, (half + t) * LANES : (half + t + 1) * LANES] = high.reshape(shape)

    for h in range(2):
        onward(drain, me, h, has_low, has_high, True)

    def finish(k, carry):
        @pl.when(k > 0)
        def _():
            relay_z(k, drain, False)

        for h in range(2):
            drain(plane_of(k) * 4 + (1 - y) * 2 + c, h, 3, c_dev)
        return carry

    lax.fori_loop(0, planes, finish, 0)

    def finish_back(s, carry):
        @pl.when(s != me)
        def _():
            for copy in back_pair(s):
                copy.wait_send()

        return carry

    lax.fori_loop(0, n, finish_back, 0)


def slot_tables(flat_probes, n, cap, clusters, per_device, probe_count):
    pair_count = flat_probes.shape[0]
    owner = flat_probes // clusters
    local = flat_probes % clusters
    pair = jnp.arange(pair_count, dtype=jnp.int32)
    same = (owner[:, None] == owner[None, :]) & (pair[None, :] < pair[:, None])
    slot = owner * cap + jnp.sum(same.astype(jnp.int32), axis=1)
    code = local * (n * per_device) + pair // probe_count
    hit = slot[None, :] == jnp.arange(n * cap, dtype=jnp.int32)[:, None]
    table = jnp.sum(jnp.where(hit, code[None, :], 0), axis=1)
    return (owner << 16) | (local << 8) | (slot - owner * cap), table


def fused_body(queries, probes, passages, centroids, counts):
    n = lax.axis_size("owner")
    per_device, probe_count = probes.shape
    clusters, span, width = passages.shape
    cap = 2 * per_device * probe_count // n
    flat = probes.reshape(-1)
    codes, table = slot_tables(flat, n, cap, clusters, per_device, probe_count)
    lane_count = 4 * cap
    count_row = jnp.pad(counts, (0, lane_count - clusters)).reshape(1, 1, lane_count)
    meta = jnp.concatenate([table.reshape(n // 4, 1, lane_count), count_row], axis=0)
    vmem = pl.BlockSpec(memory_space=pltpu.VMEM)
    smem = pl.BlockSpec(memory_space=pltpu.SMEM)
    dma = pltpu.SemaphoreType.DMA
    rows = n * per_device
    parts = span // LANES
    return pl.pallas_call(
        lambda *refs: owner_kernel(n, *refs),
        out_shape=(
            jax.ShapeDtypeStruct((per_device, probe_count, span), jnp.float32),
            jax.ShapeDtypeStruct((per_device,), jnp.int32),
        ),
        in_specs=[vmem, vmem, smem, pl.BlockSpec(memory_space=pl.ANY), vmem, smem],
        out_specs=(vmem, smem),
        scratch_shapes=[
            pltpu.VMEM((clusters, span, width), jnp.bfloat16),
            pltpu.VMEM((n, per_device, width), jnp.bfloat16),
            pltpu.VMEM((n, n // 4 + 1, 1, lane_count), jnp.int32),
            pltpu.VMEM((clusters * rows, parts, LANES), jnp.float32),
            pltpu.VMEM((4 * cap, parts, LANES), jnp.float32),
            pltpu.VMEM((n * cap, parts // 2, LANES), jnp.int32),
            pltpu.VMEM((n // 4, 1, lane_count), jnp.float32),
            pltpu.VMEM((n * cap, parts // 2, LANES), jnp.int32),
            pltpu.VMEM((n, 1, lane_count), jnp.float32),
            pltpu.VMEM((per_device * probe_count, parts // 2, LANES), jnp.int32),
            pltpu.VMEM((per_device * probe_count, 1, LANES), jnp.float32),
            pltpu.SMEM((n, 1, lane_count), jnp.int32),
            pltpu.SMEM((n, 1, lane_count), jnp.int32),
            pltpu.SMEM((n, 1, lane_count), jnp.float32),
            dma((clusters,)),
            dma((n, 2, 4)),
            dma((n, 4)),
            dma((n, 2)),
            dma((n,)),
            dma((n,)),
            dma((n,)),
            dma((n,)),
            dma((n,)),
            dma((n // 4,)),
        ],
        compiler_params=pltpu.CompilerParams(
            collective_id=0, has_side_effects=True, vmem_limit_bytes=48 * 2**20
        ),
    )(queries, meta, codes, passages, centroids, counts)


def body(queries, probes, passages, centroids, counts):
    n = lax.axis_size("owner")
    per_device, probe_count = probes.shape
    clusters, span, width = passages.shape
    lane_count = 8 * per_device * probe_count // n
    held = clusters * span * (2 * width + 4 * n * per_device) + 2 * n * per_device * width
    fits = (
        n % 4 == 0 and n >= 8 and lane_count % LANES == 0 and lane_count >= clusters
        and span % (2 * LANES) == 0 and clusters <= 256
        and lane_count <= 1024 and per_device % 32 == 0 and held < 32 * 2**20
    )
    chosen = fused_body if fits else routed_body
    return chosen(queries, probes, passages, centroids, counts)


def solution(mesh):
    in_specs = (
        P(("groups", "owner"), None),
        P(("groups", "owner"), None),
        P("owner", None, None),
        P("owner", None),
        P("owner"),
    )
    out_specs = (P(("groups", "owner"), None, None), P(("groups", "owner")))
    return jax.shard_map(body, mesh=mesh, in_specs=in_specs, out_specs=out_specs, check_vma=False)
```

```python
import jax
import jax.numpy as jnp
from jax import lax
from jax.experimental import pallas as pl
from jax.experimental.pallas import tpu as pltpu
from jax.sharding import PartitionSpec as P


def routed_body(queries, probes, passages, centroids, counts):
    owner_count = lax.axis_size("owner")
    per_device, probe_count = probes.shape
    local_count, block_span, feature_width = passages.shape
    capacity = 2 * per_device * probe_count // owner_count
    pair_count = per_device * probe_count
    passage_blocks = jnp.transpose(passages, (0, 2, 1))
    flat_probes = probes.reshape(-1)
    target_owner = flat_probes // local_count
    target_local = flat_probes % local_count
    owner_hits = (
        target_owner[:, None] == jnp.arange(owner_count, dtype=jnp.int32)[None, :]
    ).astype(jnp.int32)
    slot_rank = jnp.sum((jnp.cumsum(owner_hits, axis=0) - owner_hits) * owner_hits, axis=1)
    slot_index = target_owner * capacity + slot_rank
    pair_ids = jnp.arange(pair_count, dtype=jnp.int32)
    slot_match = slot_index[None, :] == jnp.arange(owner_count * capacity, dtype=jnp.int32)[:, None]
    slot_filled = jnp.any(slot_match, axis=1)
    source_pair = jnp.sum(jnp.where(slot_match, pair_ids[None, :], 0), axis=1)
    send_rows = jnp.where(
        slot_filled[:, None], queries[source_pair // probe_count], jnp.zeros((), jnp.bfloat16)
    )
    send_ids = jnp.where(slot_filled, target_local[source_pair], -1)
    query_rows = lax.all_to_all(
        send_rows.reshape(owner_count, capacity, feature_width),
        "owner",
        split_axis=0,
        concat_axis=0,
        tiled=True,
    )
    cluster_ids = lax.all_to_all(
        send_ids.reshape(owner_count, capacity), "owner", split_axis=0, concat_axis=0, tiled=True
    )
    source_count, slot_count = cluster_ids.shape
    row_total = source_count * slot_count
    flat_rows = query_rows.reshape(row_total, feature_width)
    flat_ids = cluster_ids.reshape(-1)
    group_ids = jnp.where(flat_ids < 0, 0, flat_ids).astype(jnp.int32)
    cluster_pick = flat_ids[:, None] == jnp.arange(local_count, dtype=jnp.int32)[None, :]
    live_sizes = jnp.sum(jnp.where(cluster_pick, counts[None, :], 0), axis=1)
    group_pick = group_ids[:, None] == jnp.arange(local_count, dtype=jnp.int32)[None, :]
    group_sizes = jnp.sum(group_pick.astype(jnp.int32), axis=0)
    order = jnp.argsort(group_ids, stable=True)
    undo_order = jnp.argsort(order, stable=True)
    sorted_rows = flat_rows[order]
    sorted_scores = lax.ragged_dot(
        sorted_rows, passage_blocks, group_sizes, preferred_element_type=jnp.float32
    )
    own_scores = sorted_scores[undo_order]
    centre_term = jnp.einsum(
        "rd,rd->r", flat_rows, centroids[group_ids], preferred_element_type=jnp.float32
    )
    live_mask = jnp.arange(block_span, dtype=jnp.int32)[None, :] < live_sizes[:, None]
    masked_scores = jnp.where(live_mask, own_scores + centre_term[:, None], 0.0)
    back_scores = lax.all_to_all(
        masked_scores.reshape(source_count, slot_count, block_span),
        "owner",
        split_axis=0,
        concat_axis=0,
        tiled=True,
    )
    back_sizes = lax.all_to_all(
        live_sizes.astype(jnp.float32).reshape(source_count, slot_count),
        "owner",
        split_axis=0,
        concat_axis=0,
        tiled=True,
    )
    flat_scores = back_scores.reshape(owner_count * capacity, block_span)
    scores = flat_scores[slot_index].reshape(per_device, probe_count, block_span)
    pair_sizes = back_sizes.reshape(-1)[slot_index].reshape(per_device, probe_count)
    visits = jnp.sum(pair_sizes, axis=1).astype(jnp.int32)
    return (scores, visits)


LANES = 128
TOP = 32767.0


def owner_kernel(
    n, q_ref, meta_ref, code_ref, pass_ref, cent_ref, cnt_ref,
    out_ref, vis_ref,
    pass_v, qs, ms, dense, picked, sendb, sends, recvb, recvs, words, factors, code_s, cnt_s, scale_s,
    pass_sem, qsend, msend, qrecv, mrecv, bsend, ssend, brecv, srecv, loc_sem,
):
    clusters, span, width = pass_ref.shape
    per_device, probe_count, _ = out_ref.shape
    planes = n // 4
    rows = n * per_device
    meta_rows, _, lane_count = meta_ref.shape
    cap = lane_count // 4
    parts = span // LANES
    half = parts // 2
    piece = per_device // 2
    me = lax.axis_index("owner")
    z = me // 4
    y = (me // 2) % 2
    c = me % 2
    y_dev = z * 4 + (1 - y) * 2 + c
    c_dev = z * 4 + y * 2 + (1 - c)
    has_low = z > 0
    has_high = z < planes - 1

    for k in range(clusters):
        pltpu.make_async_copy(pass_ref.at[k], pass_v.at[k], pass_sem.at[k]).start()

    barrier = pltpu.get_barrier_semaphore()

    def greet(dev):
        pl.semaphore_signal(barrier, inc=1, device_id={"owner": dev})

    greet(y_dev)
    greet(c_dev)

    @pl.when(has_low)
    def _():
        greet(me - 4)

    @pl.when(has_high)
    def _():
        greet(me + 4)

    pl.semaphore_wait(barrier, 2 + jnp.where(has_low, 1, 0) + jnp.where(has_high, 1, 0))

    def pair(s, h, target, dev, own=False):
        cut = pl.ds(h * piece, piece)
        query_copy = pltpu.make_async_remote_copy(
            src_ref=q_ref.at[cut] if own else qs.at[s, cut], dst_ref=qs.at[s, cut],
            send_sem=qsend.at[s, h, target], recv_sem=qrecv.at[s, h], device_id={"owner": dev},
        )
        if h == 0:
            return (query_copy,)
        return (
            query_copy,
            pltpu.make_async_remote_copy(
                src_ref=meta_ref if own else ms.at[s], dst_ref=ms.at[s],
                send_sem=msend.at[s, target], recv_sem=mrecv.at[s], device_id={"owner": dev},
            ),
        )

    def push(s, h, target, dev, own=False):
        for copy in pair(s, h, target, dev, own):
            copy.start()

    def drain(s, h, target, dev, own=False):
        for copy in pair(s, h, target, dev, own):
            copy.wait_send()

    def arrive(s, h):
        for copy in pair(s, h, 0, c_dev):
            copy.wait_recv()

    def onward(act, s, h, low, high, own=False):
        @pl.when(low)
        def _():
            act(s, h, 0, me - 4, own)

        @pl.when(high)
        def _():
            act(s, h, 1, me + 4, own)

        act(s, h, 2, y_dev, own)
        act(s, h, 3, c_dev, own)

    for h in range(2):
        onward(push, me, h, has_low, has_high, True)
    qs[me] = q_ref[...]
    ms[me] = meta_ref[...]

    near = jnp.minimum(z, planes - 1 - z)
    long_side = jnp.where(z < planes - 1 - z, 1, -1)

    def plane_of(k):
        both = jnp.where(k % 2 == 1, -1, 1) * ((k + 1) // 2)
        return z + jnp.where(k <= 2 * near, both, long_side * (k - near))

    def relay_z(k, act=push, wait=True):
        p = plane_of(k)
        s = p * 4 + y * 2 + c
        for h in range(2):
            if wait:
                arrive(s, h)
            onward(act, s, h, (p > z) & has_low, (p < z) & has_high)

    def relay_y(k):
        s = plane_of(k) * 4 + (1 - y) * 2 + c
        for h in range(2):
            arrive(s, h)
            push(s, h, 3, c_dev)

    def back_pair(s):
        return (
            pltpu.make_async_remote_copy(
                src_ref=sendb.at[pl.ds(s * cap, cap)], dst_ref=recvb.at[pl.ds(me * cap, cap)],
                send_sem=bsend.at[s], recv_sem=brecv.at[me], device_id={"owner": s},
            ),
            pltpu.make_async_remote_copy(
                src_ref=sends.at[s // 4], dst_ref=recvs.at[me],
                send_sem=ssend.at[s], recv_sem=srecv.at[me], device_id={"owner": s},
            ),
        )

    my_lane = (me % 4) * cap
    my_lanes = pl.ds(pl.multiple_of(my_lane // LANES * LANES, LANES), LANES)
    my_rest = my_lane % LANES

    def to_scalar(p):
        return pltpu.make_async_copy(
            ms.at[pl.ds(p * 4, 4), me // 4, :, my_lanes], code_s.at[pl.ds(p * 4, 4)], loc_sem.at[p]
        )

    def multiply():
        block = qs[...].reshape(rows, width)
        centre = lax.dot_general(
            block, cent_ref[...], (((1,), (1,)), ((), ())), preferred_element_type=jnp.float32
        )
        lane = lax.broadcasted_iota(jnp.int32, centre.shape, 1)
        slot_lane = lax.broadcasted_iota(jnp.int32, (1, span), 1)

        def one_cluster(cl, carry):
            pltpu.make_async_copy(pass_ref.at[cl], pass_v.at[cl], pass_sem.at[cl]).wait()
            direct = lax.dot_general(
                qs[...].reshape(rows, width), pass_v[cl],
                (((1,), (1,)), ((), ())), preferred_element_type=jnp.float32,
            )
            term = jnp.sum(jnp.where(lane == cl, centre, 0.0), axis=1, keepdims=True)
            scored = jnp.where(slot_lane < cnt_ref[cl], direct + term, 0.0)
            for t in range(parts):
                dense[pl.ds(cl * rows, rows), t, :] = scored[:, t * LANES : (t + 1) * LANES]
            return carry

        lax.fori_loop(0, clusters, one_cluster, 0)

    def compute(k):
        p = plane_of(planes - 1 - k)
        base = p * 4
        to_scalar(p).wait()
        for i in range(4):
            code_lane = my_rest

            def eight(g, carry):
                for u in range(8):
                    k_slot = g * 8 + u
                    row = code_s[base + i, 0, code_lane + k_slot] + (base + i) * per_device
                    picked[i * cap + k_slot] = dense[row]
                return carry

            lax.fori_loop(0, cap // 8, eight, 0)
        found = [picked[:, t, :] for t in range(parts)]
        peak = jnp.abs(found[0])
        for t in range(1, parts):
            peak = jnp.maximum(peak, jnp.abs(found[t]))
        top = jnp.maximum(jnp.max(peak, axis=1, keepdims=True), 1e-30)
        gain = TOP / top
        coded = [jnp.round(part * gain).astype(jnp.int32) for part in found]
        for t in range(half):
            sendb[pl.ds(base * cap, 4 * cap), t, :] = (coded[half + t] << 16) | (coded[t] & 0xFFFF)
        wide = jnp.broadcast_to(top * (1.0 / TOP), (4 * cap, LANES))
        sends[p] = jnp.transpose(wide)[0:1, :]
        for i in range(4):
            s = base + i

            @pl.when(s == me)
            def _():
                recvb[pl.ds(me * cap, cap)] = sendb[pl.ds(me * cap, cap)]
                recvs[me] = sends[p]

            @pl.when(s != me)
            def _():
                for copy in back_pair(s):
                    copy.start()

    ahead = 1 + jnp.where(near >= 1, 1, 0)

    def step(k, carry):
        @pl.when((k == 0) & (planes > 1))
        def _():
            relay_z(1)

        @pl.when((k == 0) & (ahead > 1))
        def _():
            relay_z(2)

        @pl.when((k > 0) & (k + ahead < planes))
        def _():
            relay_z(k + ahead)

        relay_y(k)
        p = plane_of(k)
        for h in range(2):
            arrive(p * 4 + y * 2 + (1 - c), h)
            arrive(p * 4 + (1 - y) * 2 + (1 - c), h)
        to_scalar(p).start()
        return carry

    lax.fori_loop(0, planes, step, 0)
    multiply()

    def answer(k, carry):
        compute(k)
        return carry

    lax.fori_loop(0, planes, answer, 0)

    def collect(s, carry):
        @pl.when(s != me)
        def _():
            for copy in (
                pltpu.make_async_remote_copy(
                    src_ref=sendb.at[pl.ds(s * cap, cap)], dst_ref=recvb.at[pl.ds(s * cap, cap)],
                    send_sem=bsend.at[s], recv_sem=brecv.at[s], device_id={"owner": c_dev},
                ),
                pltpu.make_async_remote_copy(
                    src_ref=sends.at[s // 4], dst_ref=recvs.at[s],
                    send_sem=ssend.at[s], recv_sem=srecv.at[s], device_id={"owner": c_dev},
                ),
            ):
                copy.wait_recv()

        return carry

    def count_query(q, carry):
        visited = jnp.int32(0)
        for j in range(probe_count):
            code = code_ref[q * probe_count + j]
            visited = visited + cnt_s[code >> 16, 0, (code >> 8) & 255]
        vis_ref[q] = visited
        return carry

    count_copy = pltpu.make_async_copy(ms.at[:, meta_rows - 1, :, pl.ds(0, LANES)], cnt_s, loc_sem.at[0])
    count_copy.start()
    count_copy.wait()
    lax.fori_loop(0, per_device, count_query, 0)
    lax.fori_loop(0, n, collect, 0)
    scale_copy = pltpu.make_async_copy(recvs.at[:, :, my_lanes], scale_s, loc_sem.at[0])
    scale_copy.start()
    scale_copy.wait()
    scale_lane = my_rest

    def pick_query(q, carry):
        for j in range(probe_count):
            code = code_ref[q * probe_count + j]
            kept = code & 255
            words[q * probe_count + j] = recvb[(code >> 16) * cap + kept]
            factors[q * probe_count + j] = jnp.full(
                (1, LANES), scale_s[code >> 16, 0, scale_lane + kept], jnp.float32
            )
        return carry

    lax.fori_loop(0, per_device, pick_query, 0)
    factor = factors[:, 0, :]
    for t in range(half):
        word = words[:, t, :]
        low = ((word << 16) >> 16).astype(jnp.float32) * factor
        high = (word >> 16).astype(jnp.float32) * factor
        shape = (per_device, probe_count, LANES)
        out_ref[:, :, t * LANES : (t + 1) * LANES] = low.reshape(shape)
        out_ref[:, :, (half + t) * LANES : (half + t + 1) * LANES] = high.reshape(shape)

    for h in range(2):
        onward(drain, me, h, has_low, has_high, True)

    def finish(k, carry):
        @pl.when(k > 0)
        def _():
            relay_z(k, drain, False)

        for h in range(2):
            drain(plane_of(k) * 4 + (1 - y) * 2 + c, h, 3, c_dev)
        return carry

    lax.fori_loop(0, planes, finish, 0)

    def finish_back(s, carry):
        @pl.when(s != me)
        def _():
            for copy in back_pair(s):
                copy.wait_send()

        return carry

    lax.fori_loop(0, n, finish_back, 0)


def slot_tables(flat_probes, n, cap, clusters, per_device, probe_count):
    pair_count = flat_probes.shape[0]
    owner = flat_probes // clusters
    local = flat_probes % clusters
    pair = jnp.arange(pair_count, dtype=jnp.int32)
    same = (owner[:, None] == owner[None, :]) & (pair[None, :] < pair[:, None])
    slot = owner * cap + jnp.sum(same.astype(jnp.int32), axis=1)
    code = local * (n * per_device) + pair // probe_count
    hit = slot[None, :] == jnp.arange(n * cap, dtype=jnp.int32)[:, None]
    table = jnp.sum(jnp.where(hit, code[None, :], 0), axis=1)
    return (owner << 16) | (local << 8) | (slot - owner * cap), table


def fused_body(queries, probes, passages, centroids, counts):
    n = lax.axis_size("owner")
    per_device, probe_count = probes.shape
    clusters, span, width = passages.shape
    cap = 2 * per_device * probe_count // n
    flat = probes.reshape(-1)
    codes, table = slot_tables(flat, n, cap, clusters, per_device, probe_count)
    lane_count = 4 * cap
    count_row = jnp.pad(counts, (0, lane_count - clusters)).reshape(1, 1, lane_count)
    meta = jnp.concatenate([table.reshape(n // 4, 1, lane_count), count_row], axis=0)
    vmem = pl.BlockSpec(memory_space=pltpu.VMEM)
    smem = pl.BlockSpec(memory_space=pltpu.SMEM)
    dma = pltpu.SemaphoreType.DMA
    rows = n * per_device
    parts = span // LANES
    return pl.pallas_call(
        lambda *refs: owner_kernel(n, *refs),
        out_shape=(
            jax.ShapeDtypeStruct((per_device, probe_count, span), jnp.float32),
            jax.ShapeDtypeStruct((per_device,), jnp.int32),
        ),
        in_specs=[vmem, vmem, smem, pl.BlockSpec(memory_space=pl.ANY), vmem, smem],
        out_specs=(vmem, smem),
        scratch_shapes=[
            pltpu.VMEM((clusters, span, width), jnp.bfloat16),
            pltpu.VMEM((n, per_device, width), jnp.bfloat16),
            pltpu.VMEM((n, n // 4 + 1, 1, lane_count), jnp.int32),
            pltpu.VMEM((clusters * rows, parts, LANES), jnp.float32),
            pltpu.VMEM((4 * cap, parts, LANES), jnp.float32),
            pltpu.VMEM((n * cap, parts // 2, LANES), jnp.int32),
            pltpu.VMEM((n // 4, 1, lane_count), jnp.float32),
            pltpu.VMEM((n * cap, parts // 2, LANES), jnp.int32),
            pltpu.VMEM((n, 1, lane_count), jnp.float32),
            pltpu.VMEM((per_device * probe_count, parts // 2, LANES), jnp.int32),
            pltpu.VMEM((per_device * probe_count, 1, LANES), jnp.float32),
            pltpu.SMEM((n, 1, LANES), jnp.int32),
            pltpu.SMEM((n, 1, LANES), jnp.int32),
            pltpu.SMEM((n, 1, LANES), jnp.float32),
            dma((clusters,)),
            dma((n, 2, 4)),
            dma((n, 4)),
            dma((n, 2)),
            dma((n,)),
            dma((n,)),
            dma((n,)),
            dma((n,)),
            dma((n,)),
            dma((n // 4,)),
        ],
        compiler_params=pltpu.CompilerParams(
            collective_id=0, has_side_effects=True, vmem_limit_bytes=48 * 2**20
        ),
    )(queries, meta, codes, passages, centroids, counts)


def body(queries, probes, passages, centroids, counts):
    n = lax.axis_size("owner")
    per_device, probe_count = probes.shape
    clusters, span, width = passages.shape
    lane_count = 8 * per_device * probe_count // n
    held = clusters * span * (2 * width + 4 * n * per_device) + 2 * n * per_device * width
    fits = (
        n % 4 == 0 and n >= 8 and lane_count % LANES == 0 and lane_count >= clusters
        and span % (2 * LANES) == 0 and clusters <= LANES and LANES % (lane_count // 4) == 0
        and lane_count <= 1024 and per_device % 32 == 0 and held < 32 * 2**20
    )
    chosen = fused_body if fits else routed_body
    return chosen(queries, probes, passages, centroids, counts)


def solution(mesh):
    in_specs = (
        P(("groups", "owner"), None),
        P(("groups", "owner"), None),
        P("owner", None, None),
        P("owner", None),
        P("owner"),
    )
    out_specs = (P(("groups", "owner"), None, None), P(("groups", "owner")))
    return jax.shard_map(body, mesh=mesh, in_specs=in_specs, out_specs=out_specs, check_vma=False)
```
